128 devices in a mesh: seq: 8 (over x, core), span: 16 (over y, z).
Axes of the slice: x: 4, y: 4, z: 4, core: 2. Of those that a mesh axis runs over, the one named last changes fastest.
Arguments:
- llm_input: bfloat16 [1024, 5120], P(('seq', 'span')), may hold values from -6 to 6
- hidden_grad: bfloat16 [1024, 32768], P(None, ('seq', 'span')), may hold values from -1.5 to 1.5
- gate_act: bfloat16 [1024, 32768], P(None, ('seq', 'span')), may hold values from -6 to 6
- up_weight: bfloat16 [5120, 32768], P(None, ('seq', 'span')), may hold values from -0.078125 to 0.078125
- span_counts: int32 [32], replicated, may hold values from 16 to 48, as said below
- row_ticks: int32 [1024], replicated, may hold values from 0 to 47, as said below
- encoder_out: bfloat16 [16, 384, 1280], P('span'), may hold values from -6 to 6
- mlp_input: bfloat16 [16, 384, 1280], P('span'), may hold values from -6 to 6
- post_gain: float32 [1280], replicated, may hold values from 0.5 to 1.5
- post_bias: float32 [1280], replicated, may hold values from -3 to 3
- adapter_in: bfloat16 [5120, 5120], P(None, 'seq'), may hold values from -0.078125 to 0.078125
- adapter_out: bfloat16 [5120, 5120], P('seq'), may hold values from -0.078125 to 0.078125
- expand_weight: bfloat16 [1280, 5120], P(None, 'seq'), may hold values from -0.15625 to 0.15625
- expand_bias: float32 [5120], P('seq'), may hold values from -3 to 3
- contract_weight: bfloat16 [5120, 1280], P('seq'), may hold values from -0.078125 to 0.078125
Outputs:
- gate_act_grad: bfloat16 [1024, 32768], P(None, ('seq', 'span'))
- up_weight_grad: bfloat16 [5120, 32768], P(None, ('seq', 'span'))
- adapter_in_grad: bfloat16 [5120, 5120], P('span', 'seq')
- adapter_out_grad: bfloat16 [5120, 5120], P(('seq', 'span'))
- expand_weight_grad: bfloat16 [1280, 5120], P('span', 'seq')
- contract_weight_grad: bfloat16 [5120, 1280], P(('seq', 'span'))
- expand_bias_grad: float32 [5120], P('seq')
- post_gain_grad: float32 [1280], replicated
- post_bias_grad: float32 [1280], replicated
- contract_bias_grad: float32 [1280], replicated
- encoder_out_grad: bfloat16 [16, 384, 1280], P('span', 'seq')
- mlp_input_grad: bfloat16 [16, 384, 1280], P('span', 'seq')
The draws below stay inside these ranges and needn't reach their ends.
Inputs may be any that keep to these rules, and one draw needn't show every extreme that they name: span_counts sums to 1024; its largest entry is exactly 48. `row_ticks`: the rows of each span are consecutive in the sequence, spans in order of their number, span k holding span_counts[k] rows; inside a span the tick rises by one from row to row.
All inputs are finite; a program needn't handle non-finite values.
Results may differ from the reference program's by a relative error of at most 0.03.
Values may be sent and summed in bfloat16 or wider, within the bound.
No kernel may reach another device: no remote copies, remote signals or barrier semaphores. Data moves between devices by JAX's collectives and lax.ppermute only.
A program may use at most 192 MiB of HBM per device.

```python
import math
import jax
import jax.numpy as jnp
from jax import lax

D = 5120
FF = 32768
AH = 5120
EW = 1280
EF = 5120
STACK = 4
CH_DEV = 2
ROWS = 1024
NCHUNK = 32
CAP = 48
OWN_FR = 384
AIN = 5120
N_SPAN = 16


def span_layout(key):
    mean_count = ROWS // NCHUNK
    spread = CAP - mean_count
    pair_count = NCHUNK // 2
    key_moves, key_pick, key_order, key_shift = jax.random.split(jax.random.fold_in(key, 11), 4)
    transfer = jax.random.randint(key_moves, (pair_count,), -spread, spread + 1)
    chosen = jax.random.randint(key_pick, (), 0, pair_count)
    transfer = jnp.where(jnp.arange(pair_count) == chosen, spread, transfer)
    counts = jnp.stack([mean_count + transfer, mean_count - transfer], axis=1).reshape(NCHUNK)
    counts = jax.random.permutation(key_order, counts).astype(jnp.int32)
    offsets = jax.random.randint(key_shift, (NCHUNK,), 0, CAP - counts + 1)
    span_ends = jnp.cumsum(counts)
    starts = span_ends - counts
    positions = jnp.arange(ROWS)
    span_index = jnp.sum((positions[:, None] >= span_ends[None, :]).astype(jnp.int32), axis=1)
    tick_values = offsets[span_index] + positions - starts[span_index]
    return (counts.astype(jnp.int32), tick_values.astype(jnp.int32))


def draw_span_counts(key, part):
    return span_layout(key)[0]


def draw_row_ticks(key, part):
    return span_layout(key)[1]


def steps_of(own_key, extent, cuts, least, largest):
    level = 1.0
    for position, blocks in cuts:
        heights = jax.random.uniform(jax.random.fold_in(jax.random.fold_in(own_key, 6), position), (blocks,), jnp.float32, least / len(cuts), largest / len(cuts))
        level = level * jnp.repeat(jnp.exp(heights), extent[position] // blocks).reshape((-1,) + (1,) * (len(extent) - 1 - position))
    return level


def centred(own_key, shape, scale, most, shards=(), kind=jnp.bfloat16):
    result = scale * jax.random.normal(own_key, shape, jnp.float32)
    if shards:
        result = result * steps_of(own_key, shape, shards, -0.22, 0.18)
    return jnp.clip(result, -most, most).astype(kind)


def setup_inputs(seed: int = 0) -> dict:
    keys = jax.random.split(jax.random.key(seed), 16)
    return {
        "llm_input": centred(keys[0], (ROWS, D), 1.0, 6.0, ((0, 128),)),
        "hidden_grad": centred(keys[1], (ROWS, FF), 0.25, 1.5, ((1, 128),)),
        "gate_act": centred(keys[2], (ROWS, FF), 1.0, 6.0, ((1, 128),)),
        "up_weight": centred(keys[3], (D, FF), D ** -0.5, 0.078125, ((1, 128),)),
        "span_counts": draw_span_counts(jax.random.fold_in(keys[15], 71), 0),
        "row_ticks": draw_row_ticks(jax.random.fold_in(keys[15], 71), 0),
        "encoder_out": centred(keys[6], (N_SPAN, OWN_FR, EW), 1.0, 6.0, ((0, 16),)),
        "mlp_input": centred(keys[7], (N_SPAN, OWN_FR, EW), 1.0, 6.0, ((0, 16),)),
        "post_gain": jnp.clip(1.0 + 0.1 * jax.random.normal(keys[8], (EW,), jnp.float32), 0.5, 1.5),
        "post_bias": centred(keys[9], (EW,), 0.5, 3.0, (), jnp.float32),
        "adapter_in": centred(keys[10], (AIN, AH), AIN ** -0.5, 0.078125, ((1, 8),)),
        "adapter_out": centred(keys[11], (AH, D), AH ** -0.5, 0.078125, ((0, 8),)),
        "expand_weight": centred(keys[12], (EW, EF), EW ** -0.5, 0.15625, ((1, 8),)),
        "expand_bias": centred(keys[13], (EF,), 0.5, 3.0, ((0, 8),), jnp.float32),
        "contract_weight": centred(keys[14], (EF, EW), EF ** -0.5, 0.078125, ((0, 8),)),
    }


EPSILON = 1e-05

def gelu_value(values):
    return 0.5 * values * (1.0 + lax.erf(values * (1.0 / math.sqrt(2.0))))

def gelu_slope(values):
    cumulative = 0.5 * (1.0 + lax.erf(values * (1.0 / math.sqrt(2.0))))
    return cumulative + values * jnp.exp(-0.5 * values * values) * (1.0 / math.sqrt(2.0 * math.pi))

def locate_rows(span_counts, row_ticks, capacity):
    span_ends = jnp.cumsum(span_counts).astype(jnp.int32)
    positions = jnp.arange(row_ticks.shape[0], dtype=jnp.int32)
    span_of = lax.optimization_barrier(jnp.sum((positions[:, None] >= span_ends[None, :]).astype(jnp.int32), axis=1))
    return (span_of * capacity + row_ticks).astype(jnp.int32)

def reference(llm_input, hidden_grad, gate_act, up_weight, span_counts, row_ticks, encoder_out, mlp_input, post_gain, post_bias, adapter_in, adapter_out, expand_weight, expand_bias, contract_weight):
    up_rows = jnp.dot(llm_input, up_weight, preferred_element_type=jnp.float32)
    gate_act_grad = (hidden_grad.astype(jnp.float32) * up_rows).astype(jnp.bfloat16)
    up_grad = (hidden_grad.astype(jnp.float32) * gate_act.astype(jnp.float32)).astype(jnp.bfloat16)
    up_weight_grad = jnp.dot(llm_input.T, up_grad, preferred_element_type=jnp.float32).astype(jnp.bfloat16)
    audio_grad = jnp.dot(up_grad, up_weight.T, preferred_element_type=jnp.float32).astype(jnp.bfloat16)
    groups, frames_each, width = encoder_out.shape
    slots_each = frames_each // STACK
    capacity = slots_each // CH_DEV
    slot_of = locate_rows(span_counts, row_ticks, capacity)
    token_grad = jnp.zeros((groups * slots_each, audio_grad.shape[1]), jnp.bfloat16).at[slot_of].set(audio_grad)
    frames = encoder_out.reshape(groups * frames_each, width).astype(jnp.float32)
    centre = frames - lax.optimization_barrier(jnp.mean(frames, axis=1, keepdims=True))
    rstd = lax.rsqrt(lax.optimization_barrier(jnp.mean(centre * centre, axis=1, keepdims=True)) + EPSILON)
    nhat = centre * rstd
    stacked = (nhat * post_gain + post_bias).reshape(groups * slots_each, STACK * width).astype(jnp.bfloat16)
    pre_act = jnp.dot(stacked, adapter_in, preferred_element_type=jnp.float32)
    activity = gelu_value(pre_act).astype(jnp.bfloat16)
    act_grad = jnp.dot(token_grad, adapter_out.T, preferred_element_type=jnp.float32)
    pre_grad = (act_grad * gelu_slope(pre_act)).astype(jnp.bfloat16)
    normed_grad = jnp.dot(pre_grad, adapter_in.T, preferred_element_type=jnp.float32).reshape(groups * frames_each, width)
    post_gain_grad = lax.optimization_barrier(jnp.sum(normed_grad * nhat, axis=0))
    post_bias_grad = lax.optimization_barrier(jnp.sum(normed_grad, axis=0))
    scaled = normed_grad * post_gain
    resid = rstd * (scaled - lax.optimization_barrier(jnp.mean(scaled, axis=1, keepdims=True)) - nhat * lax.optimization_barrier(jnp.mean(scaled * nhat, axis=1, keepdims=True)))
    resid = resid.astype(jnp.bfloat16)
    contract_bias_grad = lax.optimization_barrier(jnp.sum(resid.astype(jnp.float32), axis=0))
    inputs = mlp_input.reshape(groups * frames_each, width)
    hidden_pre = jnp.dot(inputs, expand_weight, preferred_element_type=jnp.float32) + expand_bias
    hidden_act = gelu_value(hidden_pre).astype(jnp.bfloat16)
    hidden_grad_enc = jnp.dot(resid, contract_weight.T, preferred_element_type=jnp.float32)
    hidden_pre_grad = (hidden_grad_enc * gelu_slope(hidden_pre)).astype(jnp.bfloat16)
    expand_bias_grad = lax.optimization_barrier(jnp.sum(hidden_pre_grad.astype(jnp.float32), axis=0))
    mlp_input_grad = jnp.dot(hidden_pre_grad, expand_weight.T, preferred_element_type=jnp.float32).astype(jnp.bfloat16)
    members = (stacked.reshape(groups, slots_each, -1), pre_grad.reshape(groups, slots_each, -1), activity.reshape(groups, slots_each, -1), token_grad.reshape(groups, slots_each, -1), inputs.reshape(groups, frames_each, -1), hidden_pre_grad.reshape(groups, frames_each, -1), hidden_act.reshape(groups, frames_each, -1), resid.reshape(groups, frames_each, -1))

    def by_group(totals, pieces):
        st_rows, pg_rows, ac_rows, tg_rows, in_rows, hp_rows, ha_rows, re_rows = pieces
        terms = (jnp.dot(st_rows.T, pg_rows, preferred_element_type=jnp.float32), jnp.dot(ac_rows.T, tg_rows, preferred_element_type=jnp.float32), jnp.dot(in_rows.T, hp_rows, preferred_element_type=jnp.float32), jnp.dot(ha_rows.T, re_rows, preferred_element_type=jnp.float32))
        updated = tuple((total + lax.optimization_barrier(term.astype(jnp.bfloat16)).astype(jnp.float32) for total, term in zip(totals, terms)))
        return (updated, None)
    start = (jnp.zeros(adapter_in.shape, jnp.float32), jnp.zeros(adapter_out.shape, jnp.float32), jnp.zeros(expand_weight.shape, jnp.float32), jnp.zeros(contract_weight.shape, jnp.float32))
    sums, _ = lax.scan(by_group, start, members)
    adapter_in_grad = sums[0].astype(jnp.bfloat16)
    adapter_out_grad = sums[1].astype(jnp.bfloat16)
    expand_weight_grad = sums[2].astype(jnp.bfloat16)
    contract_weight_grad = sums[3].astype(jnp.bfloat16)
    return (gate_act_grad, up_weight_grad, adapter_in_grad, adapter_out_grad, expand_weight_grad, contract_weight_grad, expand_bias_grad, post_gain_grad, post_bias_grad, contract_bias_grad, resid.reshape(groups, frames_each, width), mlp_input_grad.reshape(groups, frames_each, width))
```

```python
import math

import jax
import jax.numpy as jnp
from jax import lax
from jax.experimental import pallas as pl
from jax.experimental.pallas import tpu as pltpu
from jax.sharding import PartitionSpec as P

STACK = 4
CH_DEV = 2


EPSILON = 1e-05


def exchanged(pieces, axis):
    return lax.all_to_all(pieces, axis, 0, 0, tiled=True)


def sent_and_summed(shard, axis):
    size = lax.axis_size(axis)
    pieces = exchanged(shard.reshape(size, shard.shape[0] // size, *shard.shape[1:]), axis)
    return jnp.sum(pieces.astype(jnp.float32), axis=0)


def of_everyone(shard, axis):
    copies = jnp.broadcast_to(shard, (lax.axis_size(axis), *shard.shape))
    return jnp.sum(exchanged(copies, axis), axis=0)


def gelu_value(values):
    return 0.5 * values * (1.0 + lax.erf(values * (1.0 / math.sqrt(2.0))))


def gelu_slope(values):
    cumulative = 0.5 * (1.0 + lax.erf(values * (1.0 / math.sqrt(2.0))))
    return cumulative + values * jnp.exp(-0.5 * values * values) * (1.0 / math.sqrt(2.0 * math.pi))


def locate_rows(span_counts, row_ticks, capacity):
    span_ends = jnp.cumsum(span_counts)
    positions = jnp.arange(row_ticks.shape[0], dtype=jnp.int32)
    span_of = jnp.sum((positions[:, None] >= span_ends[None, :]).astype(jnp.int32), axis=1)
    return span_of * capacity + row_ticks


def contract_last(left, right):
    return lax.dot_general(
        left, right, (((1,), (1,)), ((), ())), preferred_element_type=jnp.float32
    )


def contract_first(left, right):
    return lax.dot_general(
        left, right, (((0,), (0,)), ((), ())), preferred_element_type=jnp.float32
    )


def column_block_kernel(grad_ref, weight_ref, out_ref):
    out_ref[0] = contract_last(grad_ref[...], weight_ref[...]).astype(out_ref.dtype)


def column_blocks(grad, weight, blocks):
    rows, inner = grad.shape
    width = weight.shape[0] // blocks
    return pl.pallas_call(
        column_block_kernel,
        grid=(blocks,),
        in_specs=[
            pl.BlockSpec((rows, inner), lambda i: (0, 0)),
            pl.BlockSpec((width, inner), lambda i: (i, 0)),
        ],
        out_specs=pl.BlockSpec((1, rows, width), lambda i: (i, 0, 0)),
        out_shape=jax.ShapeDtypeStruct((blocks, rows, width), jnp.bfloat16),
        cost_estimate=pl.CostEstimate(
            flops=2 * rows * inner * width * blocks,
            bytes_accessed=2 * (rows * inner + blocks * width * (inner + rows)),
            transcendentals=0,
        ),
        name="column_blocks",
    )(grad, weight)


def normalized(frames):
    centre = frames - jnp.mean(frames, axis=1, keepdims=True)
    rstd = lax.rsqrt(jnp.mean(centre * centre, axis=1, keepdims=True) + EPSILON)
    return centre * rstd, rstd


def per_device(
    llm_input,
    hidden_grad,
    gate_act,
    up_weight,
    span_counts,
    row_ticks,
    encoder_out,
    mlp_input,
    post_gain,
    post_bias,
    adapter_in,
    adapter_out,
    expand_weight,
    expand_bias,
    contract_weight,
):
    rows_all = row_ticks.shape[0]
    seq_size = lax.axis_size("seq")
    owner_count = lax.axis_size("span")
    seq_index = lax.axis_index("seq")
    frames_each = encoder_out.shape[1]
    width = encoder_out.shape[2]
    slots_each = frames_each // STACK
    capacity = slots_each // CH_DEV
    total_slots = owner_count * slots_each
    mine_frames = frames_each // seq_size

    piece = lax.all_gather(llm_input, ("seq", "span"), axis=0, tiled=True)
    up_grad = (hidden_grad.astype(jnp.float32) * gate_act.astype(jnp.float32)).astype(jnp.bfloat16)
    blocks = column_blocks(up_grad, up_weight, seq_size)
    partial_rows = lax.psum_scatter(
        blocks.reshape(seq_size * rows_all, blocks.shape[2]),
        "seq",
        scatter_dimension=0,
        tiled=True,
    )

    slot_of = locate_rows(span_counts, row_ticks, capacity)
    matches = jnp.arange(total_slots, dtype=jnp.int32)[:, None] == slot_of[None, :]
    placing = matches.astype(jnp.bfloat16)
    nhat, _ = normalized(encoder_out[0].astype(jnp.float32))
    stacked = (nhat * post_gain + post_bias).reshape(slots_each, STACK * width).astype(jnp.bfloat16)
    pre_act = jnp.dot(stacked, adapter_in, preferred_element_type=jnp.float32)
    activity = gelu_value(pre_act).astype(jnp.bfloat16)
    act_slope = gelu_slope(pre_act)
    stacked_cols = exchanged(
        jnp.moveaxis(stacked.reshape(slots_each, owner_count, -1), 1, 0), "span"
    ).reshape(total_slots, -1)
    inputs = mlp_input[0]
    hidden_pre = jnp.dot(inputs, expand_weight, preferred_element_type=jnp.float32) + expand_bias
    hidden_act = gelu_value(hidden_pre).astype(jnp.bfloat16)
    hidden_slope = gelu_slope(hidden_pre)
    mine = lax.dynamic_slice_in_dim(encoder_out[0], seq_index * mine_frames, mine_frames, 0)
    nhat_mine, rstd_mine = normalized(mine.astype(jnp.float32))
    (
        partial_rows,
        placing,
        activity,
        act_slope,
        stacked_cols,
        hidden_act,
        hidden_slope,
        nhat_mine,
        rstd_mine,
    ) = lax.optimization_barrier(
        (
            partial_rows,
            placing,
            activity,
            act_slope,
            stacked_cols,
            hidden_act,
            hidden_slope,
            nhat_mine,
            rstd_mine,
        )
    )

    partial_slots = jnp.dot(placing, partial_rows, preferred_element_type=jnp.float32)
    partial_slots, piece = lax.optimization_barrier((partial_slots.astype(jnp.bfloat16), piece))
    owned = exchanged(partial_slots.reshape(owner_count, slots_each, -1), "span")
    up_rows = jnp.dot(piece, up_weight, preferred_element_type=jnp.float32)
    gate_act_grad = (hidden_grad.astype(jnp.float32) * up_rows).astype(jnp.bfloat16)
    up_weight_grad = contract_first(piece, up_grad).astype(jnp.bfloat16)
    owned, gate_act_grad, up_weight_grad = lax.optimization_barrier(
        (owned, gate_act_grad, up_weight_grad)
    )
    token_block = jnp.sum(owned.astype(jnp.float32), axis=0).astype(jnp.bfloat16)
    token_grad = lax.all_gather(token_block, "seq", axis=1, tiled=True)

    pre_grad = (contract_last(token_grad, adapter_out) * act_slope).astype(jnp.bfloat16)
    pre_grad_all = lax.all_gather(pre_grad, "span", axis=0, tiled=True)
    normed_part = contract_last(pre_grad, adapter_in).astype(jnp.bfloat16)
    normed_part, activity = lax.optimization_barrier((normed_part, activity))
    normed_grad = sent_and_summed(normed_part.reshape(frames_each, width), "seq")
    adapter_out_grad = lax.psum_scatter(
        contract_first(activity, token_grad).astype(jnp.bfloat16),
        "span",
        scatter_dimension=0,
        tiled=True,
    )

    scaled = normed_grad * post_gain
    resid_mine = rstd_mine * (
        scaled
        - jnp.mean(scaled, axis=1, keepdims=True)
        - nhat_mine * jnp.mean(scaled * nhat_mine, axis=1, keepdims=True)
    )
    resid_mine = resid_mine.astype(jnp.bfloat16)
    resid = lax.all_gather(resid_mine, "seq", axis=0, tiled=True)

    contract_part = contract_first(hidden_act, resid).astype(jnp.bfloat16)
    contract_part, resid = lax.optimization_barrier((contract_part, resid))
    contract_weight_grad = sent_and_summed(contract_part, "span").astype(jnp.bfloat16)
    hidden_pre_grad = (contract_last(resid, contract_weight) * hidden_slope).astype(jnp.bfloat16)
    expand_part = contract_first(inputs, hidden_pre_grad).astype(jnp.bfloat16)
    expand_part, hidden_pre_grad = lax.optimization_barrier((expand_part, hidden_pre_grad))
    expand_weight_grad = sent_and_summed(expand_part, "span").astype(jnp.bfloat16)
    mlp_part = contract_last(hidden_pre_grad, expand_weight).astype(jnp.bfloat16)
    mlp_part, hidden_pre_grad, stacked_cols, normed_grad = lax.optimization_barrier(
        (mlp_part, hidden_pre_grad, stacked_cols, normed_grad)
    )
    mlp_input_grad = sent_and_summed(mlp_part, "seq").astype(jnp.bfloat16)
    expand_bias_grad = of_everyone(jnp.sum(hidden_pre_grad.astype(jnp.float32), axis=0), "span")
    adapter_in_grad = contract_first(stacked_cols, pre_grad_all).astype(jnp.bfloat16)
    sums = lax.psum(
        jnp.stack(
            [
                jnp.sum(normed_grad * nhat_mine, axis=0),
                jnp.sum(normed_grad, axis=0),
                jnp.sum(resid_mine.astype(jnp.float32), axis=0),
            ]
        ),
        ("seq", "span"),
    )
    post_gain_grad, post_bias_grad, contract_bias_grad = sums[0], sums[1], sums[2]
    return (
        gate_act_grad,
        up_weight_grad,
        adapter_in_grad,
        adapter_out_grad,
        expand_weight_grad,
        contract_weight_grad,
        expand_bias_grad,
        post_gain_grad,
        post_bias_grad,
        contract_bias_grad,
        resid_mine.reshape(1, mine_frames, width),
        mlp_input_grad.reshape(1, mine_frames, width),
    )


def solution(mesh):
    return jax.shard_map(
        per_device,
        mesh=mesh,
        in_specs=(
            P(("seq", "span"), None),
            P(None, ("seq", "span")),
            P(None, ("seq", "span")),
            P(None, ("seq", "span")),
            P(),
            P(),
            P("span", None, None),
            P("span", None, None),
            P(),
            P(),
            P(None, "seq"),
            P("seq", None),
            P(None, "seq"),
            P("seq"),
            P("seq", None),
        ),
        out_specs=(
            P(None, ("seq", "span")),
            P(None, ("seq", "span")),
            P("span", "seq"),
            P(("seq", "span"), None),
            P("span", "seq"),
            P(("seq", "span"), None),
            P("seq"),
            P(),
            P(),
            P(),
            P("span", "seq", None),
            P("span", "seq", None),
        ),
        check_vma=False,
    )
```

```python
import math

import jax
import jax.numpy as jnp
from jax import lax
from jax.experimental import pallas as pl
from jax.experimental.pallas import tpu as pltpu
from jax.sharding import PartitionSpec as P


STACK = 4
CH_DEV = 2


EPSILON = 1e-05


def exchanged(pieces, axis):
    return lax.all_to_all(pieces, axis, 0, 0, tiled=True)


def sent_and_summed(shard, axis):
    size = lax.axis_size(axis)
    pieces = exchanged(shard.reshape(size, shard.shape[0] // size, *shard.shape[1:]), axis)
    return jnp.sum(pieces.astype(jnp.float32), axis=0)


def permuted_sum(pieces, axis):
    size = lax.axis_size(axis)
    index = lax.axis_index(axis)
    mine = lax.dynamic_index_in_dim(pieces, index, 0, keepdims=False)
    arrived = []
    for step in range(1, size):
        piece = lax.dynamic_index_in_dim(pieces, (index + step) % size, 0, keepdims=False)
        arrived.append(lax.ppermute(piece, axis, [(i, (i + step) % size) for i in range(size)]))
    total = mine.astype(jnp.float32)
    for piece in arrived:
        total = total + piece.astype(jnp.float32)
    return total


def place_columns_kernel(span_ref, *refs):
    pieces, out_ref = refs[:-1], refs[-1]
    count = len(pieces)
    width = pieces[0].shape[1]
    for step in range(count):
        block = lax.rem(span_ref[0] + (count - step), count)
        out_ref[:, pl.ds(pl.multiple_of(block * width, width), width)] = pieces[step][...]


def rows_of_hidden(product, seq_size, owner_count):
    group = owner_count // 2
    rows = product.shape[0] // group
    width = product.shape[1]
    seq_index = lax.axis_index("seq")
    pieces = product.reshape(group, rows, width)
    arrived = []
    for step in range(group):
        chunk = lax.dynamic_index_in_dim(pieces, (seq_index + step) % group, 0, keepdims=False)
        pairs = []
        for s in range(seq_size):
            for k in range(owner_count):
                place = (k // 2) * owner_count + group * (k % 2) + (s + step) % group
                pairs.append((s * owner_count + k, place))
        arrived.append(lax.ppermute(chunk, ("seq", "span"), pairs))
    return pl.pallas_call(
        place_columns_kernel,
        in_specs=[pl.BlockSpec(memory_space=pltpu.SMEM)]
        + [pl.BlockSpec(memory_space=pltpu.VMEM)] * group,
        out_specs=pl.BlockSpec(memory_space=pltpu.VMEM),
        out_shape=jax.ShapeDtypeStruct((rows, group * width), product.dtype),
        cost_estimate=pl.CostEstimate(
            flops=rows * width * group, bytes_accessed=4 * rows * width * group, transcendentals=0
        ),
        name="place_columns",
    )(lax.axis_index("span").astype(jnp.int32).reshape(1), *arrived)


def gelu_value(values):
    return 0.5 * values * (1.0 + lax.erf(values * (1.0 / math.sqrt(2.0))))


def gelu_slope(values):
    cumulative = 0.5 * (1.0 + lax.erf(values * (1.0 / math.sqrt(2.0))))
    return cumulative + values * jnp.exp(-0.5 * values * values) * (1.0 / math.sqrt(2.0 * math.pi))


def locate_rows(span_counts, row_ticks, capacity):
    span_ends = jnp.cumsum(span_counts)
    positions = jnp.arange(row_ticks.shape[0], dtype=jnp.int32)
    span_of = jnp.sum((positions[:, None] >= span_ends[None, :]).astype(jnp.int32), axis=1)
    return span_of * capacity + row_ticks


def contract_last(left, right):
    return lax.dot_general(
        left, right, (((1,), (1,)), ((), ())), preferred_element_type=jnp.float32
    )


def contract_first(left, right):
    return lax.dot_general(
        left, right, (((0,), (0,)), ((), ())), preferred_element_type=jnp.float32
    )


def column_block_kernel(grad_ref, weight_ref, out_ref):
    out_ref[0] = contract_last(grad_ref[...], weight_ref[...]).astype(out_ref.dtype)


def column_blocks(grad, weight, blocks):
    rows, inner = grad.shape
    width = weight.shape[0] // blocks
    return pl.pallas_call(
        column_block_kernel,
        grid=(blocks,),
        in_specs=[
            pl.BlockSpec((rows, inner), lambda i: (0, 0)),
            pl.BlockSpec((width, inner), lambda i: (i, 0)),
        ],
        out_specs=pl.BlockSpec((1, rows, width), lambda i: (i, 0, 0)),
        out_shape=jax.ShapeDtypeStruct((blocks, rows, width), jnp.bfloat16),
        cost_estimate=pl.CostEstimate(
            flops=2 * rows * inner * width * blocks,
            bytes_accessed=2 * (rows * inner + blocks * width * (inner + rows)),
            transcendentals=0,
        ),
        name="column_blocks",
    )(grad, weight)


def normalized(frames):
    centre = frames - jnp.mean(frames, axis=1, keepdims=True)
    rstd = lax.rsqrt(jnp.mean(centre * centre, axis=1, keepdims=True) + EPSILON)
    return centre * rstd, rstd


def step(
    llm_input,
    hidden_grad,
    gate_act,
    up_weight,
    span_counts,
    row_ticks,
    encoder_out,
    mlp_input,
    post_gain,
    post_bias,
    adapter_in,
    adapter_out,
    expand_weight,
    expand_bias,
    contract_weight,
):
    rows_all = row_ticks.shape[0]
    seq_size = lax.axis_size("seq")
    owner_count = lax.axis_size("span")
    seq_index = lax.axis_index("seq")
    frames_each = encoder_out.shape[1]
    width = encoder_out.shape[2]
    slots_each = frames_each // STACK
    capacity = slots_each // CH_DEV
    total_slots = owner_count * slots_each
    mine_frames = frames_each // seq_size

    piece = lax.all_gather(llm_input, ("seq", "span"), axis=0, tiled=True)
    up_grad = (hidden_grad.astype(jnp.float32) * gate_act.astype(jnp.float32)).astype(jnp.bfloat16)
    blocks = column_blocks(up_grad, up_weight, seq_size)
    partial_rows = lax.psum_scatter(
        blocks.reshape(seq_size * rows_all, blocks.shape[2]),
        "seq",
        scatter_dimension=0,
        tiled=True,
    )

    slot_of = locate_rows(span_counts, row_ticks, capacity)
    matches = jnp.arange(total_slots, dtype=jnp.int32)[:, None] == slot_of[None, :]
    placing = matches.astype(jnp.bfloat16)
    nhat, rstd = normalized(encoder_out[0].astype(jnp.float32))
    stacked = (nhat * post_gain + post_bias).reshape(slots_each, STACK * width).astype(jnp.bfloat16)
    pre_act = jnp.dot(stacked, adapter_in, preferred_element_type=jnp.float32)
    activity = gelu_value(pre_act).astype(jnp.bfloat16)
    act_slope = gelu_slope(pre_act)
    activity_all = lax.all_gather(activity, "seq", axis=0)
    halves = owner_count // seq_size
    activity_cols = jnp.moveaxis(activity_all.reshape(seq_size, slots_each, halves, -1), 2, 1)
    stacked_cols = jnp.moveaxis(stacked.reshape(slots_each, owner_count, -1), 1, 0)
    columns = exchanged(
        jnp.concatenate([stacked_cols, activity_cols.reshape(stacked_cols.shape)], axis=2), "span"
    ).reshape(total_slots, -1)
    inputs = mlp_input[0]
    hidden_pre = jnp.dot(inputs, expand_weight, preferred_element_type=jnp.float32) + expand_bias
    hidden_act = gelu_value(hidden_pre).astype(jnp.bfloat16)
    hidden_slope = gelu_slope(hidden_pre)
    (
        partial_rows,
        placing,
        act_slope,
        columns,
        hidden_act,
        hidden_slope,
        nhat,
        rstd,
    ) = lax.optimization_barrier(
        (partial_rows, placing, act_slope, columns, hidden_act, hidden_slope, nhat, rstd)
    )

    partial_slots = jnp.dot(placing, partial_rows, preferred_element_type=jnp.float32)
    token_block = sent_and_summed(partial_slots.astype(jnp.bfloat16), "span").astype(jnp.bfloat16)
    token_all = lax.all_gather(token_block, "span", axis=0, tiled=True)
    token_grad = lax.all_gather(token_block, "seq", axis=1, tiled=True)

    pre_grad = (contract_last(token_grad, adapter_out) * act_slope).astype(jnp.bfloat16)
    normed_part = contract_last(pre_grad, adapter_in).astype(jnp.bfloat16)
    normed_part, piece = lax.optimization_barrier((normed_part, piece))
    normed_pieces = exchanged(normed_part.reshape(seq_size, mine_frames, width), "seq")

    up_rows = jnp.dot(piece, up_weight, preferred_element_type=jnp.float32)
    gate_act_grad = (hidden_grad.astype(jnp.float32) * up_rows).astype(jnp.bfloat16)
    up_weight_grad = contract_first(piece, up_grad).astype(jnp.bfloat16)
    normed_pieces, gate_act_grad, up_weight_grad = lax.optimization_barrier(
        (normed_pieces, gate_act_grad, up_weight_grad)
    )

    normed_mine = jnp.sum(normed_pieces.astype(jnp.float32), axis=0).astype(jnp.bfloat16)
    normed_grad = lax.all_gather(normed_mine, "seq", axis=0, tiled=True)
    normed_grad, token_all, pre_grad = lax.optimization_barrier((normed_grad, token_all, pre_grad))
    pre_grad_all = lax.all_gather(pre_grad, "span", axis=0, tiled=True)
    scaled = normed_grad.astype(jnp.float32) * post_gain
    resid = rstd * (
        scaled
        - jnp.mean(scaled, axis=1, keepdims=True)
        - nhat * jnp.mean(scaled * nhat, axis=1, keepdims=True)
    )
    resid = resid.astype(jnp.bfloat16)

    contract_part = contract_first(hidden_act, resid).astype(jnp.bfloat16)
    contract_part, resid = lax.optimization_barrier((contract_part, resid))
    contract_pieces = exchanged(contract_part.reshape(owner_count, -1, width), "span")
    hidden_pre_grad = (contract_last(resid, contract_weight) * hidden_slope).astype(jnp.bfloat16)
    expand_part = contract_first(inputs, hidden_pre_grad).astype(jnp.bfloat16)
    expand_part, hidden_pre_grad = lax.optimization_barrier((expand_part, hidden_pre_grad))
    mlp_part = contract_last(hidden_pre_grad, expand_weight).astype(jnp.bfloat16)
    mlp_part, hidden_pre_grad, token_all, normed_grad = lax.optimization_barrier(
        (mlp_part, hidden_pre_grad, token_all, normed_grad)
    )
    expand_part, contract_pieces = lax.optimization_barrier((expand_part, contract_pieces))
    expand_pieces = exchanged(expand_part.reshape(owner_count, -1, expand_part.shape[1]), "span")
    contract_weight_grad = jnp.sum(contract_pieces.astype(jnp.float32), axis=0).astype(jnp.bfloat16)
    mlp_input_grad = permuted_sum(
        mlp_part.reshape(seq_size, mine_frames, width), "seq"
    ).astype(jnp.bfloat16)

    inner = stacked_cols.shape[2]
    out_product = contract_first(columns[:, inner:], token_all).astype(jnp.bfloat16)
    out_product, columns = lax.optimization_barrier((out_product, columns))
    adapter_out_grad = rows_of_hidden(out_product, seq_size, owner_count)
    adapter_in_grad = contract_first(columns[:, :inner], pre_grad_all).astype(jnp.bfloat16)

    normed_grad = normed_grad.astype(jnp.float32)
    sums = jnp.concatenate(
        [
            jnp.sum(normed_grad * nhat, axis=0),
            jnp.sum(normed_grad, axis=0),
            jnp.sum(resid.astype(jnp.float32), axis=0),
            jnp.sum(hidden_pre_grad.astype(jnp.float32), axis=0),
        ]
    )
    sums = jnp.sum(lax.all_gather(sums, "span", axis=0), axis=0)
    post_gain_grad, post_bias_grad, contract_bias_grad, expand_bias_grad = (
        sums[:width],
        sums[width : 2 * width],
        sums[2 * width : 3 * width],
        sums[3 * width :],
    )
    expand_weight_grad = jnp.sum(expand_pieces.astype(jnp.float32), axis=0).astype(jnp.bfloat16)
    resid_mine = lax.dynamic_slice_in_dim(resid, seq_index * mine_frames, mine_frames, 0)
    return (
        gate_act_grad,
        up_weight_grad,
        adapter_in_grad,
        adapter_out_grad,
        expand_weight_grad,
        contract_weight_grad,
        expand_bias_grad,
        post_gain_grad,
        post_bias_grad,
        contract_bias_grad,
        resid_mine.reshape(1, mine_frames, width),
        mlp_input_grad.reshape(1, mine_frames, width),
    )


def solution(mesh):
    return jax.shard_map(
        step,
        mesh=mesh,
        in_specs=(
            P(("seq", "span"), None),
            P(None, ("seq", "span")),
            P(None, ("seq", "span")),
            P(None, ("seq", "span")),
            P(),
            P(),
            P("span", None, None),
            P("span", None, None),
            P(),
            P(),
            P(None, "seq"),
            P("seq", None),
            P(None, "seq"),
            P("seq"),
            P("seq", None),
        ),
        out_specs=(
            P(None, ("seq", "span")),
            P(None, ("seq", "span")),
            P("span", "seq"),
            P(("seq", "span"), None),
            P("span", "seq"),
            P(("seq", "span"), None),
            P("seq"),
            P(),
            P(),
            P(),
            P("span", "seq", None),
            P("span", "seq", None),
        ),
        check_vma=False,
    )
```

```python
import math

import jax
import jax.numpy as jnp
from jax import lax
from jax.experimental import pallas as pl
from jax.sharding import PartitionSpec as P


STACK = 4
CH_DEV = 2


EPSILON = 1e-05


def exchanged(pieces, axis):
    return lax.all_to_all(pieces, axis, 0, 0, tiled=True)


def sent_and_summed(shard, axis):
    size = lax.axis_size(axis)
    pieces = exchanged(shard.reshape(size, shard.shape[0] // size, *shard.shape[1:]), axis)
    return jnp.sum(pieces.astype(jnp.float32), axis=0)


def permuted_sum(pieces, axis):
    size = lax.axis_size(axis)
    index = lax.axis_index(axis)
    mine = lax.dynamic_index_in_dim(pieces, index, 0, keepdims=False)
    arrived = []
    for step in range(1, size):
        piece = lax.dynamic_index_in_dim(pieces, (index + step) % size, 0, keepdims=False)
        arrived.append(lax.ppermute(piece, axis, [(i, (i + step) % size) for i in range(size)]))
    total = mine.astype(jnp.float32)
    for piece in arrived:
        total = total + piece.astype(jnp.float32)
    return total


def blocks_swapped(array, outer, inner):
    blocks = array.reshape(outer, inner, -1, array.shape[1])
    return jnp.swapaxes(blocks, 0, 1).reshape(array.shape)


def gelu_value(values):
    return 0.5 * values * (1.0 + lax.erf(values * (1.0 / math.sqrt(2.0))))


def gelu_slope(values):
    cumulative = 0.5 * (1.0 + lax.erf(values * (1.0 / math.sqrt(2.0))))
    return cumulative + values * jnp.exp(-0.5 * values * values) * (1.0 / math.sqrt(2.0 * math.pi))


def locate_rows(span_counts, row_ticks, capacity):
    span_ends = jnp.cumsum(span_counts)
    positions = jnp.arange(row_ticks.shape[0], dtype=jnp.int32)
    span_of = jnp.sum((positions[:, None] >= span_ends[None, :]).astype(jnp.int32), axis=1)
    return span_of * capacity + row_ticks


def contract_last(left, right):
    return lax.dot_general(
        left, right, (((1,), (1,)), ((), ())), preferred_element_type=jnp.float32
    )


def contract_first(left, right):
    return lax.dot_general(
        left, right, (((0,), (0,)), ((), ())), preferred_element_type=jnp.float32
    )


def column_block_kernel(hidden_ref, gate_ref, weight_ref, grad_ref, out_ref):
    @pl.when(pl.program_id(0) == 0)
    def _():
        product = hidden_ref[...].astype(jnp.float32) * gate_ref[...].astype(jnp.float32)
        grad_ref[...] = product.astype(grad_ref.dtype)

    out_ref[0] = contract_last(grad_ref[...], weight_ref[...]).astype(out_ref.dtype)


def column_blocks(hidden_grad, gate_act, weight, blocks):
    rows, inner = hidden_grad.shape
    width = weight.shape[0] // blocks
    whole = pl.BlockSpec((rows, inner), lambda i: (0, 0))
    return pl.pallas_call(
        column_block_kernel,
        grid=(blocks,),
        in_specs=[whole, whole, pl.BlockSpec((width, inner), lambda i: (i, 0))],
        out_specs=[whole, pl.BlockSpec((1, rows, width), lambda i: (i, 0, 0))],
        out_shape=[
            jax.ShapeDtypeStruct((rows, inner), jnp.bfloat16),
            jax.ShapeDtypeStruct((blocks, rows, width), jnp.bfloat16),
        ],
        cost_estimate=pl.CostEstimate(
            flops=2 * rows * inner * width * blocks,
            bytes_accessed=2 * (3 * rows * inner + blocks * width * (inner + rows)),
            transcendentals=0,
        ),
        name="column_blocks",
    )(hidden_grad, gate_act, weight)


def normalized(frames):
    centre = frames - jnp.mean(frames, axis=1, keepdims=True)
    rstd = lax.rsqrt(jnp.mean(centre * centre, axis=1, keepdims=True) + EPSILON)
    return centre * rstd, rstd


def step(
    llm_input,
    hidden_grad,
    gate_act,
    up_weight,
    span_counts,
    row_ticks,
    encoder_out,
    mlp_input,
    post_gain,
    post_bias,
    adapter_in,
    adapter_out,
    expand_weight,
    expand_bias,
    contract_weight,
):
    rows_all = row_ticks.shape[0]
    seq_size = lax.axis_size("seq")
    owner_count = lax.axis_size("span")
    seq_index = lax.axis_index("seq")
    frames_each = encoder_out.shape[1]
    width = encoder_out.shape[2]
    slots_each = frames_each // STACK
    capacity = slots_each // CH_DEV
    total_slots = owner_count * slots_each
    mine_frames = frames_each // seq_size

    piece = lax.all_gather(llm_input, "seq", axis=0, tiled=True)
    piece = lax.all_gather(piece, "span", axis=0, tiled=True)
    up_grad, blocks = column_blocks(hidden_grad, gate_act, up_weight, seq_size)
    partial_rows = lax.psum_scatter(
        blocks.reshape(seq_size * rows_all, blocks.shape[2]),
        "seq",
        scatter_dimension=0,
        tiled=True,
    )

    hidden_rows = blocks_swapped(hidden_grad, seq_size, owner_count)
    up_grad_rows = blocks_swapped(up_grad, seq_size, owner_count)

    slot_of = locate_rows(span_counts, row_ticks, capacity)
    matches = jnp.arange(total_slots, dtype=jnp.int32)[:, None] == slot_of[None, :]
    placing = matches.astype(jnp.bfloat16)
    nhat, rstd = normalized(encoder_out[0].astype(jnp.float32))
    stacked = (nhat * post_gain + post_bias).reshape(slots_each, STACK * width).astype(jnp.bfloat16)
    pre_act = jnp.dot(stacked, adapter_in, preferred_element_type=jnp.float32)
    activity = gelu_value(pre_act).astype(jnp.bfloat16)
    act_slope = gelu_slope(pre_act)
    activity_all = lax.all_gather(activity, "span", axis=0, tiled=True)
    columns = exchanged(
        jnp.moveaxis(stacked.reshape(slots_each, owner_count, -1), 1, 0), "span"
    ).reshape(total_slots, -1)
    inputs = mlp_input[0]
    hidden_pre = jnp.dot(inputs, expand_weight, preferred_element_type=jnp.float32) + expand_bias
    hidden_act = gelu_value(hidden_pre).astype(jnp.bfloat16)
    hidden_slope = gelu_slope(hidden_pre)
    (
        partial_rows,
        placing,
        act_slope,
        columns,
        hidden_act,
        hidden_slope,
        nhat,
        rstd,
        hidden_rows,
        up_grad_rows,
    ) = lax.optimization_barrier(
        (
            partial_rows,
            placing,
            act_slope,
            columns,
            hidden_act,
            hidden_slope,
            nhat,
            rstd,
            hidden_rows,
            up_grad_rows,
        )
    )

    partial_slots = jnp.dot(placing, partial_rows, preferred_element_type=jnp.float32)
    token_block = sent_and_summed(partial_slots.astype(jnp.bfloat16), "span").astype(jnp.bfloat16)
    token_grad = lax.all_gather(token_block, "seq", axis=1, tiled=True)

    pre_grad = (contract_last(token_grad, adapter_out) * act_slope).astype(jnp.bfloat16)
    normed_part = contract_last(pre_grad, adapter_in).astype(jnp.bfloat16)
    pre_grad_all = lax.all_gather(pre_grad, "span", axis=0, tiled=True)
    normed_part, token_grad, piece = lax.optimization_barrier((normed_part, token_grad, piece))
    normed_pieces = exchanged(normed_part.reshape(seq_size, mine_frames, width), "seq")

    token_cols = jnp.moveaxis(token_grad.reshape(slots_each, owner_count, -1), 1, 0)

    up_rows = jnp.dot(piece, up_weight, preferred_element_type=jnp.float32)
    gate_rows = (hidden_rows.astype(jnp.float32) * up_rows).astype(jnp.bfloat16)
    gate_act_grad = blocks_swapped(gate_rows, owner_count, seq_size)
    up_weight_grad = contract_first(piece, up_grad_rows).astype(jnp.bfloat16)
    normed_pieces, gate_act_grad, up_weight_grad, token_cols = lax.optimization_barrier(
        (normed_pieces, gate_act_grad, up_weight_grad, token_cols)
    )
    token_cols = exchanged(token_cols, "span").reshape(total_slots, -1)

    normed_mine = jnp.sum(normed_pieces.astype(jnp.float32), axis=0).astype(jnp.bfloat16)
    normed_grad = lax.all_gather(normed_mine, "seq", axis=0, tiled=True)
    scaled = normed_grad.astype(jnp.float32) * post_gain
    resid = rstd * (
        scaled
        - jnp.mean(scaled, axis=1, keepdims=True)
        - nhat * jnp.mean(scaled * nhat, axis=1, keepdims=True)
    )
    resid = resid.astype(jnp.bfloat16)

    contract_part = contract_first(hidden_act, resid).astype(jnp.bfloat16)
    contract_part, resid, token_cols = lax.optimization_barrier((contract_part, resid, token_cols))
    contract_pieces = exchanged(contract_part.reshape(owner_count, -1, width), "span")
    hidden_pre_grad = (contract_last(resid, contract_weight) * hidden_slope).astype(jnp.bfloat16)
    expand_part = contract_first(inputs, hidden_pre_grad).astype(jnp.bfloat16)
    expand_part, hidden_pre_grad, activity_all = lax.optimization_barrier(
        (expand_part, hidden_pre_grad, activity_all)
    )
    mlp_part = contract_last(hidden_pre_grad, expand_weight).astype(jnp.bfloat16)
    out_part = contract_first(activity_all, token_cols).astype(jnp.bfloat16)
    mlp_part, hidden_pre_grad, columns, normed_grad = lax.optimization_barrier(
        (mlp_part, hidden_pre_grad, columns, normed_grad)
    )
    rows = expand_part.shape[0] // owner_count
    packed = jnp.concatenate(
        [
            expand_part.reshape(owner_count, rows, -1),
            out_part.reshape(owner_count, -1, expand_part.shape[1]),
        ],
        axis=1,
    )
    packed, contract_pieces = lax.optimization_barrier((packed, contract_pieces))
    packed = exchanged(packed, "span")
    contract_weight_grad = jnp.sum(contract_pieces.astype(jnp.float32), axis=0).astype(jnp.bfloat16)
    mlp_input_grad = permuted_sum(
        mlp_part.reshape(seq_size, mine_frames, width), "seq"
    ).astype(jnp.bfloat16)

    adapter_in_grad = contract_first(columns, pre_grad_all).astype(jnp.bfloat16)

    normed_grad = normed_grad.astype(jnp.float32)
    sums = jnp.concatenate(
        [
            jnp.sum(normed_grad * nhat, axis=0),
            jnp.sum(normed_grad, axis=0),
            jnp.sum(resid.astype(jnp.float32), axis=0),
            jnp.sum(hidden_pre_grad.astype(jnp.float32), axis=0),
        ]
    )
    sums = jnp.sum(lax.all_gather(sums, "span", axis=0), axis=0)
    post_gain_grad, post_bias_grad, contract_bias_grad, expand_bias_grad = (
        sums[:width],
        sums[width : 2 * width],
        sums[2 * width : 3 * width],
        sums[3 * width :],
    )
    expand_weight_grad = jnp.sum(packed[:, :rows].astype(jnp.float32), axis=0).astype(jnp.bfloat16)
    out_rows = packed[:, rows:].reshape(owner_count, -1, out_part.shape[1])
    adapter_out_grad = jnp.moveaxis(out_rows, 0, 1).reshape(out_rows.shape[1], -1)
    resid_mine = lax.dynamic_slice_in_dim(resid, seq_index * mine_frames, mine_frames, 0)
    return (
        gate_act_grad,
        up_weight_grad,
        adapter_in_grad,
        adapter_out_grad,
        expand_weight_grad,
        contract_weight_grad,
        expand_bias_grad,
        post_gain_grad,
        post_bias_grad,
        contract_bias_grad,
        resid_mine.reshape(1, mine_frames, width),
        mlp_input_grad.reshape(1, mine_frames, width),
    )


def solution(mesh):
    return jax.shard_map(
        step,
        mesh=mesh,
        in_specs=(
            P(("seq", "span"), None),
            P(None, ("seq", "span")),
            P(None, ("seq", "span")),
            P(None, ("seq", "span")),
            P(),
            P(),
            P("span", None, None),
            P("span", None, None),
            P(),
            P(),
            P(None, "seq"),
            P("seq", None),
            P(None, "seq"),
            P("seq"),
            P("seq", None),
        ),
        out_specs=(
            P(None, ("seq", "span")),
            P(None, ("seq", "span")),
            P("span", "seq"),
            P(("seq", "span"), None),
            P("span", "seq"),
            P(("seq", "span"), None),
            P("seq"),
            P(),
            P(),
            P(),
            P("span", "seq", None),
            P("span", "seq", None),
        ),
        check_vma=False,
    )
```

```python
import math

import jax
import jax.numpy as jnp
from jax import lax
from jax.experimental import pallas as pl
from jax.sharding import PartitionSpec as P


STACK = 4
CH_DEV = 2


EPSILON = 1e-05


def exchanged(pieces, axis):
    return lax.all_to_all(pieces, axis, 0, 0, tiled=True)


def sent_and_summed(shard, axis):
    size = lax.axis_size(axis)
    pieces = exchanged(shard.reshape(size, shard.shape[0] // size, *shard.shape[1:]), axis)
    return jnp.sum(pieces.astype(jnp.float32), axis=0)


def permuted_sum(pieces, axis):
    size = lax.axis_size(axis)
    index = lax.axis_index(axis)
    mine = lax.dynamic_index_in_dim(pieces, index, 0, keepdims=False)
    arrived = []
    for step in range(1, size):
        piece = lax.dynamic_index_in_dim(pieces, (index + step) % size, 0, keepdims=False)
        arrived.append(lax.ppermute(piece, axis, [(i, (i + step) % size) for i in range(size)]))
    total = mine.astype(jnp.float32)
    for piece in arrived:
        total = total + piece.astype(jnp.float32)
    return total.astype(jnp.bfloat16)


def gelu_value(values):
    return 0.5 * values * (1.0 + lax.erf(values * (1.0 / math.sqrt(2.0))))


def gelu_slope(values):
    cumulative = 0.5 * (1.0 + lax.erf(values * (1.0 / math.sqrt(2.0))))
    return cumulative + values * jnp.exp(-0.5 * values * values) * (1.0 / math.sqrt(2.0 * math.pi))


def locate_rows(span_counts, row_ticks, capacity):
    span_ends = jnp.cumsum(span_counts)
    positions = jnp.arange(row_ticks.shape[0], dtype=jnp.int32)
    span_of = jnp.sum((positions[:, None] >= span_ends[None, :]).astype(jnp.int32), axis=1)
    return span_of * capacity + row_ticks


def contract_last(left, right):
    return lax.dot_general(
        left, right, (((1,), (1,)), ((), ())), preferred_element_type=jnp.float32
    )


def contract_first(left, right):
    return lax.dot_general(
        left, right, (((0,), (0,)), ((), ())), preferred_element_type=jnp.float32
    )


def column_block_kernel(hidden_ref, gate_ref, weight_ref, grad_ref, out_ref):
    @pl.when(pl.program_id(0) == 0)
    def _():
        product = hidden_ref[...].astype(jnp.float32) * gate_ref[...].astype(jnp.float32)
        grad_ref[...] = product.astype(grad_ref.dtype)

    out_ref[0] = contract_last(grad_ref[...], weight_ref[...]).astype(out_ref.dtype)


def column_blocks(hidden_grad, gate_act, weight, blocks):
    rows, inner = hidden_grad.shape
    width = weight.shape[0] // blocks
    whole = pl.BlockSpec((rows, inner), lambda i: (0, 0))
    return pl.pallas_call(
        column_block_kernel,
        grid=(blocks,),
        in_specs=[whole, whole, pl.BlockSpec((width, inner), lambda i: (i, 0))],
        out_specs=[whole, pl.BlockSpec((1, rows, width), lambda i: (i, 0, 0))],
        out_shape=[
            jax.ShapeDtypeStruct((rows, inner), jnp.bfloat16),
            jax.ShapeDtypeStruct((blocks, rows, width), jnp.bfloat16),
        ],
        cost_estimate=pl.CostEstimate(
            flops=2 * rows * inner * width * blocks,
            bytes_accessed=2 * (3 * rows * inner + blocks * width * (inner + rows)),
            transcendentals=0,
        ),
        name="column_blocks",
    )(hidden_grad, gate_act, weight)


def normalized(frames):
    centre = frames - jnp.mean(frames, axis=1, keepdims=True)
    rstd = lax.rsqrt(jnp.mean(centre * centre, axis=1, keepdims=True) + EPSILON)
    return centre * rstd, rstd


def step(
    llm_input,
    hidden_grad,
    gate_act,
    up_weight,
    span_counts,
    row_ticks,
    encoder_out,
    mlp_input,
    post_gain,
    post_bias,
    adapter_in,
    adapter_out,
    expand_weight,
    expand_bias,
    contract_weight,
):
    rows_all = row_ticks.shape[0]
    seq_size = lax.axis_size("seq")
    owner_count = lax.axis_size("span")
    seq_index = lax.axis_index("seq")
    frames_each = encoder_out.shape[1]
    width = encoder_out.shape[2]
    slots_each = frames_each // STACK
    capacity = slots_each // CH_DEV
    total_slots = owner_count * slots_each
    mine_frames = frames_each // seq_size

    piece = lax.all_gather(llm_input, ("seq", "span"), axis=0, tiled=True)
    up_grad, blocks = column_blocks(hidden_grad, gate_act, up_weight, seq_size)
    partial_rows = lax.psum_scatter(
        blocks.reshape(seq_size * rows_all, blocks.shape[2]),
        "seq",
        scatter_dimension=0,
        tiled=True,
    )

    slot_of = locate_rows(span_counts, row_ticks, capacity)
    matches = jnp.arange(total_slots, dtype=jnp.int32)[:, None] == slot_of[None, :]
    placing = matches.astype(jnp.bfloat16)
    nhat, rstd = normalized(encoder_out[0].astype(jnp.float32))
    stacked = (nhat * post_gain + post_bias).reshape(slots_each, STACK * width).astype(jnp.bfloat16)
    pre_act = jnp.dot(stacked, adapter_in, preferred_element_type=jnp.float32)
    activity = gelu_value(pre_act).astype(jnp.bfloat16)
    act_slope = gelu_slope(pre_act)
    activity_all = lax.all_gather(activity, "span", axis=0, tiled=True)
    columns = exchanged(
        jnp.moveaxis(stacked.reshape(slots_each, owner_count, -1), 1, 0), "span"
    ).reshape(total_slots, -1)
    inputs = mlp_input[0]
    hidden_pre = jnp.dot(inputs, expand_weight, preferred_element_type=jnp.float32) + expand_bias
    hidden_act = gelu_value(hidden_pre).astype(jnp.bfloat16)
    hidden_slope = gelu_slope(hidden_pre)
    (
        partial_rows,
        placing,
        act_slope,
        columns,
        hidden_act,
        hidden_slope,
        nhat,
        rstd,
    ) = lax.optimization_barrier(
        (
            partial_rows,
            placing,
            act_slope,
            columns,
            hidden_act,
            hidden_slope,
            nhat,
            rstd,
        )
    )

    partial_slots = jnp.dot(placing, partial_rows, preferred_element_type=jnp.float32)
    token_block = sent_and_summed(partial_slots.astype(jnp.bfloat16), "span").astype(jnp.bfloat16)
    token_grad = lax.all_gather(token_block, "seq", axis=1, tiled=True)

    pre_grad = (contract_last(token_grad, adapter_out) * act_slope).astype(jnp.bfloat16)
    pre_grad_all = lax.all_gather(pre_grad, "span", axis=0, tiled=True)
    normed_part = contract_last(pre_grad, adapter_in).astype(jnp.bfloat16)
    normed_part, token_grad, piece = lax.optimization_barrier((normed_part, token_grad, piece))
    normed_pieces = exchanged(normed_part.reshape(seq_size, mine_frames, width), "seq")

    token_cols = jnp.moveaxis(token_grad.reshape(slots_each, owner_count, -1), 1, 0)

    up_rows = jnp.dot(piece, up_weight, preferred_element_type=jnp.float32)
    gate_act_grad = (hidden_grad.astype(jnp.float32) * up_rows).astype(jnp.bfloat16)
    up_weight_grad = contract_first(piece, up_grad).astype(jnp.bfloat16)
    normed_pieces, gate_act_grad, up_weight_grad, token_cols = lax.optimization_barrier(
        (normed_pieces, gate_act_grad, up_weight_grad, token_cols)
    )
    token_cols = exchanged(token_cols, "span").reshape(total_slots, -1)

    normed_mine = jnp.sum(normed_pieces.astype(jnp.float32), axis=0).astype(jnp.bfloat16)
    normed_grad = lax.all_gather(normed_mine, "seq", axis=0, tiled=True)
    scaled = normed_grad.astype(jnp.float32) * post_gain
    resid = rstd * (
        scaled
        - jnp.mean(scaled, axis=1, keepdims=True)
        - nhat * jnp.mean(scaled * nhat, axis=1, keepdims=True)
    )
    resid = resid.astype(jnp.bfloat16)

    contract_part = contract_first(hidden_act, resid).astype(jnp.bfloat16)
    contract_part, resid, token_cols = lax.optimization_barrier((contract_part, resid, token_cols))
    contract_pieces = exchanged(contract_part.reshape(owner_count, -1, width), "span")
    hidden_pre_grad = (contract_last(resid, contract_weight) * hidden_slope).astype(jnp.bfloat16)
    expand_part = contract_first(inputs, hidden_pre_grad).astype(jnp.bfloat16)
    expand_part, hidden_pre_grad, activity_all = lax.optimization_barrier(
        (expand_part, hidden_pre_grad, activity_all)
    )
    mlp_part = contract_last(hidden_pre_grad, expand_weight).astype(jnp.bfloat16)
    out_part = contract_first(activity_all, token_cols).astype(jnp.bfloat16)
    mlp_part, hidden_pre_grad, columns, normed_grad = lax.optimization_barrier(
        (mlp_part, hidden_pre_grad, columns, normed_grad)
    )

    frame_grad = normed_grad.astype(jnp.float32)
    sums = jnp.concatenate(
        [
            jnp.sum(frame_grad * nhat, axis=0),
            jnp.sum(frame_grad, axis=0),
            jnp.sum(resid.astype(jnp.float32), axis=0),
            jnp.sum(hidden_pre_grad.astype(jnp.float32), axis=0),
        ]
    ).reshape(-1, expand_part.shape[1])
    high = lax.reduce_precision(sums, exponent_bits=8, mantissa_bits=7)
    halves = jnp.concatenate([high, sums - high]).astype(jnp.bfloat16)
    rows = expand_part.shape[0] // owner_count
    out_pieces = out_part.reshape(owner_count, -1, expand_part.shape[1])
    packed = jnp.concatenate(
        [
            expand_part.reshape(owner_count, rows, -1),
            out_pieces,
            jnp.broadcast_to(halves, (owner_count, *halves.shape)),
        ],
        axis=1,
    )
    packed, contract_pieces = lax.optimization_barrier((packed, contract_pieces))
    packed = exchanged(packed, "span")
    contract_weight_grad = jnp.sum(contract_pieces.astype(jnp.float32), axis=0).astype(jnp.bfloat16)
    mlp_input_grad = permuted_sum(mlp_part.reshape(seq_size, mine_frames, width), "seq")

    adapter_in_grad = contract_first(columns, pre_grad_all).astype(jnp.bfloat16)

    expand_weight_grad = jnp.sum(packed[:, :rows].astype(jnp.float32), axis=0).astype(jnp.bfloat16)
    out_end = rows + out_pieces.shape[1]
    out_rows = packed[:, rows:out_end].reshape(owner_count, -1, out_part.shape[1])
    adapter_out_grad = jnp.moveaxis(out_rows, 0, 1).reshape(out_rows.shape[1], -1)
    sums = jnp.sum(packed[:, out_end:].astype(jnp.float32), axis=0)
    sums = (sums[: high.shape[0]] + sums[high.shape[0] :]).reshape(-1)
    post_gain_grad, post_bias_grad, contract_bias_grad, expand_bias_grad = (
        sums[:width],
        sums[width : 2 * width],
        sums[2 * width : 3 * width],
        sums[3 * width :],
    )
    resid_mine = lax.dynamic_slice_in_dim(resid, seq_index * mine_frames, mine_frames, 0)
    return (
        gate_act_grad,
        up_weight_grad,
        adapter_in_grad,
        adapter_out_grad,
        expand_weight_grad,
        contract_weight_grad,
        expand_bias_grad,
        post_gain_grad,
        post_bias_grad,
        contract_bias_grad,
        resid_mine.reshape(1, mine_frames, width),
        mlp_input_grad.reshape(1, mine_frames, width),
    )


def solution(mesh):
    return jax.shard_map(
        step,
        mesh=mesh,
        in_specs=(
            P(("seq", "span"), None),
            P(None, ("seq", "span")),
            P(None, ("seq", "span")),
            P(None, ("seq", "span")),
            P(),
            P(),
            P("span", None, None),
            P("span", None, None),
            P(),
            P(),
            P(None, "seq"),
            P("seq", None),
            P(None, "seq"),
            P("seq"),
            P("seq", None),
        ),
        out_specs=(
            P(None, ("seq", "span")),
            P(None, ("seq", "span")),
            P("span", "seq"),
            P(("seq", "span"), None),
            P("span", "seq"),
            P(("seq", "span"), None),
            P("seq"),
            P(),
            P(),
            P(),
            P("span", "seq", None),
            P("span", "seq", None),
        ),
        check_vma=False,
    )
```

```python
import math

import jax
import jax.numpy as jnp
from jax import lax
from jax.experimental import pallas as pl
from jax.sharding import PartitionSpec as P


STACK = 4
CH_DEV = 2


EPSILON = 1e-05


def exchanged(pieces, axis):
    return lax.all_to_all(pieces, axis, 0, 0, tiled=True)


def sent_and_summed(shard, axis):
    size = lax.axis_size(axis)
    pieces = exchanged(shard.reshape(size, shard.shape[0] // size, *shard.shape[1:]), axis)
    return jnp.sum(pieces.astype(jnp.float32), axis=0)


def permuted_sum(pieces, axis):
    size = lax.axis_size(axis)
    index = lax.axis_index(axis)
    mine = lax.dynamic_index_in_dim(pieces, index, 0, keepdims=False)
    arrived = []
    for step in range(1, size):
        piece = lax.dynamic_index_in_dim(pieces, (index + step) % size, 0, keepdims=False)
        arrived.append(lax.ppermute(piece, axis, [(i, (i + step) % size) for i in range(size)]))
    total = mine.astype(jnp.float32)
    for piece in arrived:
        total = total + piece.astype(jnp.float32)
    return total.astype(jnp.bfloat16)


def gelu_value(values):
    return 0.5 * values * (1.0 + lax.erf(values * (1.0 / math.sqrt(2.0))))


def gelu_slope(values):
    cumulative = 0.5 * (1.0 + lax.erf(values * (1.0 / math.sqrt(2.0))))
    return cumulative + values * jnp.exp(-0.5 * values * values) * (1.0 / math.sqrt(2.0 * math.pi))


def locate_rows(span_counts, row_ticks, capacity):
    span_ends = jnp.cumsum(span_counts)
    positions = jnp.arange(row_ticks.shape[0], dtype=jnp.int32)
    span_of = jnp.sum((positions[:, None] >= span_ends[None, :]).astype(jnp.int32), axis=1)
    return span_of * capacity + row_ticks


def contract_last(left, right):
    return lax.dot_general(
        left, right, (((1,), (1,)), ((), ())), preferred_element_type=jnp.float32
    )


def contract_first(left, right):
    return lax.dot_general(
        left, right, (((0,), (0,)), ((), ())), preferred_element_type=jnp.float32
    )


def column_block_kernel(hidden_ref, gate_ref, weight_ref, grad_ref, out_ref):
    @pl.when(pl.program_id(0) == 0)
    def _():
        product = hidden_ref[...].astype(jnp.float32) * gate_ref[...].astype(jnp.float32)
        grad_ref[...] = product.astype(grad_ref.dtype)

    out_ref[0] = contract_last(grad_ref[...], weight_ref[...]).astype(out_ref.dtype)


def column_blocks(hidden_grad, gate_act, weight, blocks):
    rows, inner = hidden_grad.shape
    width = weight.shape[0] // blocks
    whole = pl.BlockSpec((rows, inner), lambda i: (0, 0))
    return pl.pallas_call(
        column_block_kernel,
        grid=(blocks,),
        in_specs=[whole, whole, pl.BlockSpec((width, inner), lambda i: (i, 0))],
        out_specs=[whole, pl.BlockSpec((1, rows, width), lambda i: (i, 0, 0))],
        out_shape=[
            jax.ShapeDtypeStruct((rows, inner), jnp.bfloat16),
            jax.ShapeDtypeStruct((blocks, rows, width), jnp.bfloat16),
        ],
        cost_estimate=pl.CostEstimate(
            flops=2 * rows * inner * width * blocks,
            bytes_accessed=2 * (3 * rows * inner + blocks * width * (inner + rows)),
            transcendentals=0,
        ),
        name="column_blocks",
    )(hidden_grad, gate_act, weight)


def normalized(frames):
    centre = frames - jnp.mean(frames, axis=1, keepdims=True)
    rstd = lax.rsqrt(jnp.mean(centre * centre, axis=1, keepdims=True) + EPSILON)
    return centre * rstd, rstd


def step(
    llm_input,
    hidden_grad,
    gate_act,
    up_weight,
    span_counts,
    row_ticks,
    encoder_out,
    mlp_input,
    post_gain,
    post_bias,
    adapter_in,
    adapter_out,
    expand_weight,
    expand_bias,
    contract_weight,
):
    rows_all = row_ticks.shape[0]
    seq_size = lax.axis_size("seq")
    owner_count = lax.axis_size("span")
    seq_index = lax.axis_index("seq")
    frames_each = encoder_out.shape[1]
    width = encoder_out.shape[2]
    slots_each = frames_each // STACK
    capacity = slots_each // CH_DEV
    total_slots = owner_count * slots_each
    mine_frames = frames_each // seq_size

    up_grad, blocks = column_blocks(hidden_grad, gate_act, up_weight, seq_size)
    partial_rows = lax.psum_scatter(
        blocks.reshape(seq_size * rows_all, blocks.shape[2]),
        "seq",
        scatter_dimension=0,
        tiled=True,
    )

    slot_of = locate_rows(span_counts, row_ticks, capacity)
    matches = jnp.arange(total_slots, dtype=jnp.int32)[:, None] == slot_of[None, :]
    placing = matches.astype(jnp.bfloat16)
    nhat, rstd = normalized(encoder_out[0].astype(jnp.float32))
    stacked = (nhat * post_gain + post_bias).reshape(slots_each, STACK * width).astype(jnp.bfloat16)
    pre_act = jnp.dot(stacked, adapter_in, preferred_element_type=jnp.float32)
    activity = gelu_value(pre_act).astype(jnp.bfloat16)
    act_slope = gelu_slope(pre_act)
    activity_all = lax.all_gather(activity, "span", axis=0, tiled=True)
    columns = exchanged(
        jnp.moveaxis(stacked.reshape(slots_each, owner_count, -1), 1, 0), "span"
    ).reshape(total_slots, -1)
    inputs = mlp_input[0]
    hidden_pre = jnp.dot(inputs, expand_weight, preferred_element_type=jnp.float32) + expand_bias
    hidden_act = gelu_value(hidden_pre).astype(jnp.bfloat16)
    hidden_slope = gelu_slope(hidden_pre)
    (
        partial_rows,
        placing,
        act_slope,
        columns,
        hidden_act,
        hidden_slope,
        nhat,
        rstd,
    ) = lax.optimization_barrier(
        (
            partial_rows,
            placing,
            act_slope,
            columns,
            hidden_act,
            hidden_slope,
            nhat,
            rstd,
        )
    )

    partial_slots = jnp.dot(placing, partial_rows, preferred_element_type=jnp.float32)
    token_block = sent_and_summed(partial_slots.astype(jnp.bfloat16), "span").astype(jnp.bfloat16)
    token_block, llm_input = lax.optimization_barrier((token_block, llm_input))
    piece = lax.all_gather(llm_input, ("seq", "span"), axis=0, tiled=True)
    token_grad = lax.all_gather(token_block, "seq", axis=1, tiled=True)

    pre_grad = (contract_last(token_grad, adapter_out) * act_slope).astype(jnp.bfloat16)
    pre_grad_all = lax.all_gather(pre_grad, "span", axis=0, tiled=True)
    normed_part = contract_last(pre_grad, adapter_in).astype(jnp.bfloat16)
    normed_part, token_grad = lax.optimization_barrier((normed_part, token_grad))
    normed_pieces = exchanged(normed_part.reshape(seq_size, mine_frames, width), "seq")

    token_cols = jnp.moveaxis(token_grad.reshape(slots_each, owner_count, -1), 1, 0)

    up_rows = jnp.dot(piece, up_weight, preferred_element_type=jnp.float32)
    gate_act_grad = (hidden_grad.astype(jnp.float32) * up_rows).astype(jnp.bfloat16)
    up_weight_grad = contract_first(piece, up_grad).astype(jnp.bfloat16)
    normed_pieces, token_cols = lax.optimization_barrier((normed_pieces, token_cols))
    token_cols = exchanged(token_cols, "span").reshape(total_slots, -1)

    normed_mine = jnp.sum(normed_pieces.astype(jnp.float32), axis=0).astype(jnp.bfloat16)
    normed_grad = lax.all_gather(normed_mine, "seq", axis=0, tiled=True)
    scaled = normed_grad.astype(jnp.float32) * post_gain
    resid = rstd * (
        scaled
        - jnp.mean(scaled, axis=1, keepdims=True)
        - nhat * jnp.mean(scaled * nhat, axis=1, keepdims=True)
    )
    resid = resid.astype(jnp.bfloat16)

    contract_part = contract_first(hidden_act, resid).astype(jnp.bfloat16)
    contract_part, resid, token_cols = lax.optimization_barrier((contract_part, resid, token_cols))
    contract_pieces = exchanged(contract_part.reshape(owner_count, -1, width), "span")
    hidden_pre_grad = (contract_last(resid, contract_weight) * hidden_slope).astype(jnp.bfloat16)
    expand_part = contract_first(inputs, hidden_pre_grad).astype(jnp.bfloat16)
    expand_part, hidden_pre_grad, activity_all = lax.optimization_barrier(
        (expand_part, hidden_pre_grad, activity_all)
    )
    mlp_part = contract_last(hidden_pre_grad, expand_weight).astype(jnp.bfloat16)
    out_part = contract_first(activity_all, token_cols).astype(jnp.bfloat16)
    mlp_part, hidden_pre_grad, columns, normed_grad = lax.optimization_barrier(
        (mlp_part, hidden_pre_grad, columns, normed_grad)
    )

    frame_grad = normed_grad.astype(jnp.float32)
    sums = jnp.concatenate(
        [
            jnp.sum(frame_grad * nhat, axis=0),
            jnp.sum(frame_grad, axis=0),
            jnp.sum(resid.astype(jnp.float32), axis=0),
            jnp.sum(hidden_pre_grad.astype(jnp.float32), axis=0),
        ]
    ).reshape(-1, expand_part.shape[1])
    high = lax.reduce_precision(sums, exponent_bits=8, mantissa_bits=7)
    halves = jnp.concatenate([high, sums - high]).astype(jnp.bfloat16)
    rows = expand_part.shape[0] // owner_count
    out_pieces = out_part.reshape(owner_count, -1, expand_part.shape[1])
    packed = jnp.concatenate(
        [
            expand_part.reshape(owner_count, rows, -1),
            out_pieces,
            jnp.broadcast_to(halves, (owner_count, *halves.shape)),
        ],
        axis=1,
    )
    packed, contract_pieces = lax.optimization_barrier((packed, contract_pieces))
    packed = exchanged(packed, "span")
    contract_weight_grad = jnp.sum(contract_pieces.astype(jnp.float32), axis=0).astype(jnp.bfloat16)
    mlp_input_grad = permuted_sum(mlp_part.reshape(seq_size, mine_frames, width), "seq")

    adapter_in_grad = contract_first(columns, pre_grad_all).astype(jnp.bfloat16)

    expand_weight_grad = jnp.sum(packed[:, :rows].astype(jnp.float32), axis=0).astype(jnp.bfloat16)
    out_end = rows + out_pieces.shape[1]
    out_rows = packed[:, rows:out_end].reshape(owner_count, -1, out_part.shape[1])
    adapter_out_grad = jnp.moveaxis(out_rows, 0, 1).reshape(out_rows.shape[1], -1)
    sums = jnp.sum(packed[:, out_end:].astype(jnp.float32), axis=0)
    sums = (sums[: high.shape[0]] + sums[high.shape[0] :]).reshape(-1)
    post_gain_grad, post_bias_grad, contract_bias_grad, expand_bias_grad = (
        sums[:width],
        sums[width : 2 * width],
        sums[2 * width : 3 * width],
        sums[3 * width :],
    )
    resid_mine = lax.dynamic_slice_in_dim(resid, seq_index * mine_frames, mine_frames, 0)
    return (
        gate_act_grad,
        up_weight_grad,
        adapter_in_grad,
        adapter_out_grad,
        expand_weight_grad,
        contract_weight_grad,
        expand_bias_grad,
        post_gain_grad,
        post_bias_grad,
        contract_bias_grad,
        resid_mine.reshape(1, mine_frames, width),
        mlp_input_grad.reshape(1, mine_frames, width),
    )


def solution(mesh):
    return jax.shard_map(
        step,
        mesh=mesh,
        in_specs=(
            P(("seq", "span"), None),
            P(None, ("seq", "span")),
            P(None, ("seq", "span")),
            P(None, ("seq", "span")),
            P(),
            P(),
            P("span", None, None),
            P("span", None, None),
            P(),
            P(),
            P(None, "seq"),
            P("seq", None),
            P(None, "seq"),
            P("seq"),
            P("seq", None),
        ),
        out_specs=(
            P(None, ("seq", "span")),
            P(None, ("seq", "span")),
            P("span", "seq"),
            P(("seq", "span"), None),
            P("span", "seq"),
            P(("seq", "span"), None),
            P("seq"),
            P(),
            P(),
            P(),
            P("span", "seq", None),
            P("span", "seq", None),
        ),
        check_vma=False,
    )
```

```python
import math

import jax
import jax.numpy as jnp
from jax import lax
from jax.experimental.layout import Layout, with_layout_constraint
from jax.experimental import pallas as pl
from jax.sharding import PartitionSpec as P


STACK = 4
CH_DEV = 2


EPSILON = 1e-05


def exchanged(pieces, axis):
    return lax.all_to_all(pieces, axis, 0, 0, tiled=True)


def sent_and_summed(shard, axis):
    size = lax.axis_size(axis)
    pieces = exchanged(shard.reshape(size, shard.shape[0] // size, *shard.shape[1:]), axis)
    return jnp.sum(pieces.astype(jnp.float32), axis=0)


def permuted_sum(pieces, axis):
    size = lax.axis_size(axis)
    index = lax.axis_index(axis)
    mine = lax.dynamic_index_in_dim(pieces, index, 0, keepdims=False)
    arrived = []
    for step in range(1, size):
        piece = lax.dynamic_index_in_dim(pieces, (index + step) % size, 0, keepdims=False)
        arrived.append(lax.ppermute(piece, axis, [(i, (i + step) % size) for i in range(size)]))
    total = mine.astype(jnp.float32)
    for piece in arrived:
        total = total + piece.astype(jnp.float32)
    return total.astype(jnp.bfloat16)


def gelu_value(values):
    return 0.5 * values * (1.0 + lax.erf(values * (1.0 / math.sqrt(2.0))))


def gelu_slope(values):
    cumulative = 0.5 * (1.0 + lax.erf(values * (1.0 / math.sqrt(2.0))))
    return cumulative + values * jnp.exp(-0.5 * values * values) * (1.0 / math.sqrt(2.0 * math.pi))


def locate_rows(span_counts, row_ticks, capacity):
    span_ends = jnp.cumsum(span_counts)
    positions = jnp.arange(row_ticks.shape[0], dtype=jnp.int32)
    span_of = jnp.sum((positions[:, None] >= span_ends[None, :]).astype(jnp.int32), axis=1)
    return span_of * capacity + row_ticks


def contract_last(left, right):
    return lax.dot_general(
        left, right, (((1,), (1,)), ((), ())), preferred_element_type=jnp.float32
    )


def contract_first(left, right):
    return lax.dot_general(
        left, right, (((0,), (0,)), ((), ())), preferred_element_type=jnp.float32
    )


def column_block_kernel(hidden_ref, gate_ref, weight_ref, grad_ref, out_ref):
    @pl.when(pl.program_id(0) == 0)
    def _():
        product = hidden_ref[...].astype(jnp.float32) * gate_ref[...].astype(jnp.float32)
        grad_ref[...] = product.astype(grad_ref.dtype)

    out_ref[0] = contract_last(grad_ref[...], weight_ref[...]).astype(out_ref.dtype)


def column_blocks(hidden_grad, gate_act, weight, blocks):
    rows, inner = hidden_grad.shape
    width = weight.shape[0] // blocks
    whole = pl.BlockSpec((rows, inner), lambda i: (0, 0))
    return pl.pallas_call(
        column_block_kernel,
        grid=(blocks,),
        in_specs=[whole, whole, pl.BlockSpec((width, inner), lambda i: (i, 0))],
        out_specs=[whole, pl.BlockSpec((1, rows, width), lambda i: (i, 0, 0))],
        out_shape=[
            jax.ShapeDtypeStruct((rows, inner), jnp.bfloat16),
            jax.ShapeDtypeStruct((blocks, rows, width), jnp.bfloat16),
        ],
        cost_estimate=pl.CostEstimate(
            flops=2 * rows * inner * width * blocks,
            bytes_accessed=2 * (3 * rows * inner + blocks * width * (inner + rows)),
            transcendentals=0,
        ),
        name="column_blocks",
    )(hidden_grad, gate_act, weight)


def normalized(frames):
    centre = frames - jnp.mean(frames, axis=1, keepdims=True)
    rstd = lax.rsqrt(jnp.mean(centre * centre, axis=1, keepdims=True) + EPSILON)
    return centre * rstd, rstd


def step(
    llm_input,
    hidden_grad,
    gate_act,
    up_weight,
    span_counts,
    row_ticks,
    encoder_out,
    mlp_input,
    post_gain,
    post_bias,
    adapter_in,
    adapter_out,
    expand_weight,
    expand_bias,
    contract_weight,
):
    rows_all = row_ticks.shape[0]
    seq_size = lax.axis_size("seq")
    owner_count = lax.axis_size("span")
    seq_index = lax.axis_index("seq")
    frames_each = encoder_out.shape[1]
    width = encoder_out.shape[2]
    slots_each = frames_each // STACK
    capacity = slots_each // CH_DEV
    total_slots = owner_count * slots_each
    mine_frames = frames_each // seq_size

    up_grad, blocks = column_blocks(hidden_grad, gate_act, up_weight, seq_size)
    partial_rows = lax.psum_scatter(
        blocks.reshape(seq_size * rows_all, blocks.shape[2]),
        "seq",
        scatter_dimension=0,
        tiled=True,
    )

    slot_of = locate_rows(span_counts, row_ticks, capacity)
    matches = jnp.arange(total_slots, dtype=jnp.int32)[:, None] == slot_of[None, :]
    placing = matches.astype(jnp.bfloat16)
    nhat, rstd = normalized(encoder_out[0].astype(jnp.float32))
    stacked = (nhat * post_gain + post_bias).reshape(slots_each, STACK * width).astype(jnp.bfloat16)
    pre_act = jnp.dot(stacked, adapter_in, preferred_element_type=jnp.float32)
    activity = gelu_value(pre_act).astype(jnp.bfloat16)
    act_slope = gelu_slope(pre_act)
    activity_all = lax.all_gather(activity, "span", axis=0, tiled=True)
    columns = exchanged(
        jnp.moveaxis(stacked.reshape(slots_each, owner_count, -1), 1, 0), "span"
    ).reshape(total_slots, -1)
    inputs = mlp_input[0]
    hidden_pre = jnp.dot(inputs, expand_weight, preferred_element_type=jnp.float32) + expand_bias
    hidden_act = gelu_value(hidden_pre).astype(jnp.bfloat16)
    hidden_slope = gelu_slope(hidden_pre)
    (
        partial_rows,
        placing,
        act_slope,
        columns,
        hidden_act,
        hidden_slope,
        nhat,
        rstd,
    ) = lax.optimization_barrier(
        (
            partial_rows,
            placing,
            act_slope,
            columns,
            hidden_act,
            hidden_slope,
            nhat,
            rstd,
        )
    )

    partial_slots = jnp.dot(placing, partial_rows, preferred_element_type=jnp.float32)
    token_block = sent_and_summed(partial_slots.astype(jnp.bfloat16), "span").astype(jnp.bfloat16)
    token_block, llm_input = lax.optimization_barrier((token_block, llm_input))
    piece = lax.all_gather(llm_input, ("seq", "span"), axis=0, tiled=True)
    token_grad = lax.all_gather(token_block, "seq", axis=1, tiled=True)

    pre_grad = (contract_last(token_grad, adapter_out) * act_slope).astype(jnp.bfloat16)
    pre_grad_all = lax.all_gather(pre_grad, "span", axis=0, tiled=True)
    normed_part = contract_last(pre_grad, adapter_in).astype(jnp.bfloat16)
    normed_part, token_grad = lax.optimization_barrier((normed_part, token_grad))
    normed_pieces = exchanged(normed_part.reshape(seq_size, mine_frames, width), "seq")

    token_cols = with_layout_constraint(
        jnp.moveaxis(token_grad.reshape(slots_each, owner_count, -1), 1, 0), Layout((0, 1, 2))
    )

    up_rows = jnp.dot(piece, up_weight, preferred_element_type=jnp.float32)
    gate_act_grad = (hidden_grad.astype(jnp.float32) * up_rows).astype(jnp.bfloat16)
    up_weight_grad = contract_first(piece, up_grad).astype(jnp.bfloat16)
    normed_pieces, token_cols = lax.optimization_barrier((normed_pieces, token_cols))
    token_cols = exchanged(token_cols, "span").reshape(total_slots, -1)

    normed_mine = jnp.sum(normed_pieces.astype(jnp.float32), axis=0).astype(jnp.bfloat16)
    normed_grad = lax.all_gather(normed_mine, "seq", axis=0, tiled=True)
    scaled = normed_grad.astype(jnp.float32) * post_gain
    resid = rstd * (
        scaled
        - jnp.mean(scaled, axis=1, keepdims=True)
        - nhat * jnp.mean(scaled * nhat, axis=1, keepdims=True)
    )
    resid = resid.astype(jnp.bfloat16)

    contract_part = contract_first(hidden_act, resid).astype(jnp.bfloat16)
    contract_part, resid, token_cols = lax.optimization_barrier((contract_part, resid, token_cols))
    contract_pieces = exchanged(contract_part.reshape(owner_count, -1, width), "span")
    hidden_pre_grad = (contract_last(resid, contract_weight) * hidden_slope).astype(jnp.bfloat16)
    expand_part = contract_first(inputs, hidden_pre_grad).astype(jnp.bfloat16)
    expand_part, hidden_pre_grad, activity_all = lax.optimization_barrier(
        (expand_part, hidden_pre_grad, activity_all)
    )
    mlp_part = contract_last(hidden_pre_grad, expand_weight).astype(jnp.bfloat16)
    out_part = contract_first(activity_all, token_cols).astype(jnp.bfloat16)
    mlp_part, hidden_pre_grad, columns, normed_grad = lax.optimization_barrier(
        (mlp_part, hidden_pre_grad, columns, normed_grad)
    )

    frame_grad = normed_grad.astype(jnp.float32)
    sums = jnp.concatenate(
        [
            jnp.sum(frame_grad * nhat, axis=0),
            jnp.sum(frame_grad, axis=0),
            jnp.sum(resid.astype(jnp.float32), axis=0),
            jnp.sum(hidden_pre_grad.astype(jnp.float32), axis=0),
        ]
    ).reshape(-1, expand_part.shape[1])
    high = lax.reduce_precision(sums, exponent_bits=8, mantissa_bits=7)
    halves = jnp.concatenate([high, sums - high]).astype(jnp.bfloat16)
    rows = expand_part.shape[0] // owner_count
    out_pieces = out_part.reshape(owner_count, -1, expand_part.shape[1])
    packed = jnp.concatenate(
        [
            expand_part.reshape(owner_count, rows, -1),
            out_pieces,
            jnp.broadcast_to(halves, (owner_count, *halves.shape)),
        ],
        axis=1,
    )
    packed, contract_pieces = lax.optimization_barrier((packed, contract_pieces))
    packed = exchanged(packed, "span")
    contract_weight_grad = jnp.sum(contract_pieces.astype(jnp.float32), axis=0).astype(jnp.bfloat16)
    mlp_input_grad = permuted_sum(mlp_part.reshape(seq_size, mine_frames, width), "seq")

    adapter_in_grad = contract_first(columns, pre_grad_all).astype(jnp.bfloat16)

    expand_weight_grad = jnp.sum(packed[:, :rows].astype(jnp.float32), axis=0).astype(jnp.bfloat16)
    out_end = rows + out_pieces.shape[1]
    out_rows = packed[:, rows:out_end].reshape(owner_count, -1, out_part.shape[1])
    adapter_out_grad = jnp.moveaxis(out_rows, 0, 1).reshape(out_rows.shape[1], -1)
    sums = jnp.sum(packed[:, out_end:].astype(jnp.float32), axis=0)
    sums = (sums[: high.shape[0]] + sums[high.shape[0] :]).reshape(-1)
    post_gain_grad, post_bias_grad, contract_bias_grad, expand_bias_grad = (
        sums[:width],
        sums[width : 2 * width],
        sums[2 * width : 3 * width],
        sums[3 * width :],
    )
    resid_mine = lax.dynamic_slice_in_dim(resid, seq_index * mine_frames, mine_frames, 0)
    return (
        gate_act_grad,
        up_weight_grad,
        adapter_in_grad,
        adapter_out_grad,
        expand_weight_grad,
        contract_weight_grad,
        expand_bias_grad,
        post_gain_grad,
        post_bias_grad,
        contract_bias_grad,
        resid_mine.reshape(1, mine_frames, width),
        mlp_input_grad.reshape(1, mine_frames, width),
    )


def solution(mesh):
    return jax.shard_map(
        step,
        mesh=mesh,
        in_specs=(
            P(("seq", "span"), None),
            P(None, ("seq", "span")),
            P(None, ("seq", "span")),
            P(None, ("seq", "span")),
            P(),
            P(),
            P("span", None, None),
            P("span", None, None),
            P(),
            P(),
            P(None, "seq"),
            P("seq", None),
            P(None, "seq"),
            P("seq"),
            P("seq", None),
        ),
        out_specs=(
            P(None, ("seq", "span")),
            P(None, ("seq", "span")),
            P("span", "seq"),
            P(("seq", "span"), None),
            P("span", "seq"),
            P(("seq", "span"), None),
            P("seq"),
            P(),
            P(),
            P(),
            P("span", "seq", None),
            P("span", "seq", None),
        ),
        check_vma=False,
    )
```
